512 devices in a mesh: slab: 32 (over z, core), sub: 16 (over x, y).
Axes of the slice: x: 4, y: 4, z: 16, core: 2. Of those that a mesh axis runs over, the one named last changes fastest.
Arguments:
- child_moments: bfloat16 [216, 524288], P(None, ('slab', 'sub')), may hold values from -6 to 6
- incoming: bfloat16 [216, 65536], P(None, ('slab', 'sub')), may hold values from -6 to 6
- m2m_ops: bfloat16 [8, 216, 216], replicated, may hold values from -0.15625 to 0.15625
- m2l_ops: bfloat16 [160, 216, 216], P('sub'), may hold values from -0.046875 to 0.046875
- l2l_ops: bfloat16 [8, 216, 216], replicated, may hold values from -0.4375 to 0.4375
- partners: int32 [160, 65536], P(None, ('slab', 'sub')), may hold values from -1 to 65535, as said below
Outputs:
- child_locals: float32 [216, 524288], P(None, ('slab', 'sub'))
The draws below stay inside these ranges and needn't reach their ends.
Inputs may be any that keep to these rules, and one draw needn't show every extreme that they name: `partners`: cells are numbered in Morton order of bricks of the domain, each brick one cell wide along the first dimension; the source of a pair lies in the same slab as its target or in an adjacent one, that is its id divided by 128 * 16 differs from the target's by at most one. Pairs are those of the interaction list: source and target are not adjacent, their parents are.
All inputs are finite; a program needn't handle non-finite values.
Results may differ from the reference program's by a relative error of at most 0.0035.
Values may be sent and summed in bfloat16 or wider, within the bound.
A program may use at most 128 MiB of HBM per device.

```python
import math
import jax
import jax.numpy as jnp
import numpy as np
from jax import lax

W = 216
OPS = 160
CELLS_DEV = 128
CELLS = 65536
LEAVES = 524288
N_SLAB = 32
N_SUB = 16


def offset_rows():
    forced = [(2, 0, 0), (-2, 0, 0), (1, 0, 2), (-1, 0, 2)]
    entries = list(forced)
    for first in range(-3, 4):
        for second in range(-3, 4):
            for third in range(-3, 4):
                if max(abs(first), abs(second), abs(third)) > 1 and (first, second, third) not in forced:
                    entries.append((first, second, third))
    return np.array(entries, np.int32)


def draw_partners(key, part):
    table_all = jnp.asarray(offset_rows())
    rest_count = table_all.shape[0] - 4
    chosen = jnp.concatenate([jnp.arange(4, dtype=jnp.int32), 4 + jax.random.permutation(key, rest_count)[:OPS - 4].astype(jnp.int32)])
    shifts = table_all[chosen]
    side_x = math.isqrt(N_SUB)
    side_y = N_SUB // side_x
    brick_depth = CELLS_DEV // 16
    cell_total = CELLS_DEV * N_SLAB * N_SUB
    cell_ids = jnp.arange(cell_total, dtype=jnp.int32)
    device_ids = cell_ids // CELLS_DEV
    inner_ids = cell_ids % CELLS_DEV
    slab_ids = device_ids // N_SUB
    sub_ids = device_ids % N_SUB
    pos_x = sub_ids // side_y
    pos_y = sub_ids % side_y * 16 + inner_ids % 2 + 2 * (inner_ids // 2 % 2) + 4 * (inner_ids // 8 % 2) + 8 * (inner_ids // 16 % 2)
    pos_z = slab_ids * brick_depth + inner_ids // 4 % 2 + 2 * (inner_ids // 32 % 2) + 4 * (inner_ids // 64)
    far_x = pos_x[None, :] + shifts[:, 0:1]
    far_y = pos_y[None, :] + shifts[:, 1:2]
    far_z = pos_z[None, :] + shifts[:, 2:3]
    inside = (far_x >= 0) & (far_x < side_x) & (far_y >= 0) & (far_y < 16 * side_y)
    inside = inside & (far_z >= 0) & (far_z < brick_depth * N_SLAB)
    near = jnp.abs(jnp.floor_divide(far_x, 2) - pos_x[None, :] // 2) <= 1
    near = near & (jnp.abs(jnp.floor_divide(far_y, 2) - pos_y[None, :] // 2) <= 1)
    near = near & (jnp.abs(jnp.floor_divide(far_z, 2) - pos_z[None, :] // 2) <= 1)
    safe_x = jnp.clip(far_x, 0, side_x - 1)
    safe_y = jnp.clip(far_y, 0, 16 * side_y - 1)
    safe_z = jnp.clip(far_z, 0, brick_depth * N_SLAB - 1)
    loc_y = safe_y % 16
    loc_z = safe_z % brick_depth
    inner_new = loc_y % 2 + 2 * (loc_y // 2 % 2) + 4 * (loc_z % 2) + 8 * (loc_y // 4 % 2) + 16 * (loc_y // 8 % 2)
    inner_new = inner_new + 32 * (loc_z // 2 % 2) + 64 * (loc_z // 4)
    device_new = safe_z // brick_depth * N_SUB + safe_x * side_y + safe_y // 16
    source_ids = device_new * CELLS_DEV + inner_new
    return jnp.where(inside & near, source_ids, -1).astype(jnp.int32)


def block_levels(stream_key, shape, split, least, top_value):
    level = 1.0
    for axis_at, blocks in split:
        draws = jax.random.uniform(jax.random.fold_in(jax.random.fold_in(stream_key, 6), axis_at), (blocks,), jnp.float32, least / len(split), top_value / len(split))
        level = level * jnp.repeat(jnp.exp(draws), shape[axis_at] // blocks).reshape((-1,) + (1,) * (len(shape) - 1 - axis_at))
    return level


def gaussian(key, dims, width, reach, shards=(), held_as=jnp.bfloat16):
    result = jax.random.normal(key, dims, jnp.float32) * width
    if len(shards) > 0:
        result = block_levels(key, dims, shards, -0.22, 0.18) * result
    return jnp.clip(result, min=-reach, max=reach).astype(held_as)


def setup_inputs(seed: int = 0) -> dict:
    streams_of = jax.random.split(jax.random.key(seed), 7)
    return {
        "child_moments": gaussian(streams_of[0], (W, LEAVES), 1.0, 6.0, ((1, 512),)),
        "incoming": gaussian(streams_of[1], (W, CELLS), 1.0, 6.0, ((1, 512),)),
        "m2m_ops": gaussian(streams_of[2], (8, W, W), (8 * W) ** -0.5, 0.15625),
        "m2l_ops": gaussian(streams_of[3], (OPS, W, W), (W * OPS // 2) ** -0.5, 0.046875, ((0, 16),)),
        "l2l_ops": gaussian(streams_of[4], (8, W, W), W ** -0.5, 0.4375),
        "partners": draw_partners(jax.random.fold_in(streams_of[6], 71), 0),
    }


def reference(child_moments, incoming, m2m_ops, m2l_ops, l2l_ops, partners):
    order_cube = child_moments.shape[0]
    cell_count = child_moments.shape[1] // 8
    children = child_moments.astype(jnp.float32).reshape(order_cube, cell_count, 8)
    moments = jnp.einsum("oij,jpo->ip", m2m_ops.astype(jnp.float32), children).astype(jnp.bfloat16)

    def apply_op(summed, operand_pair):
        op_matrix, source_row = operand_pair
        usable = source_row >= 0
        columns = jnp.take(moments, jnp.where(usable, source_row, 0).astype(jnp.int32), axis=1)
        columns = jnp.where(usable[None, :], columns, jnp.zeros((), jnp.bfloat16))
        return summed + jnp.dot(op_matrix, columns, preferred_element_type=jnp.float32), None

    far_field, _ = lax.scan(apply_op, jnp.zeros((order_cube, cell_count), jnp.float32), (m2l_ops, partners))
    locals_all = (incoming.astype(jnp.float32) + far_field).astype(jnp.bfloat16)
    child_out = jnp.einsum("oij,jp->ipo", l2l_ops.astype(jnp.float32), locals_all.astype(jnp.float32))
    return child_out.reshape(order_cube, cell_count * 8)
```

```python
import functools

import jax
import jax.numpy as jnp
from jax import lax
from jax.experimental import pallas as pl
from jax.experimental.pallas import tpu as pltpu
from jax.sharding import PartitionSpec as P

MESH = pl.DeviceIdType.MESH
F32 = jnp.float32
BF16 = jnp.bfloat16
VM = pl.BlockSpec(memory_space=pltpu.VMEM)
NONE = 64


def peers_of(sub, n_sub):
    side = 4
    steps = [(dx, dy) for dx in range(side) for dy in range(n_sub // side) if (dx, dy) != (0, 0)]
    steps.sort(key=lambda s: min(s[0], 4 - s[0]) + min(s[1], 4 - s[1]))
    return steps


def moved(sub, step, sign):
    x, y = sub // 4, sub % 4
    return (x + sign * step[0] + 4) % 4 * 4 + (y + sign * step[1] + 4) % 4


def exchange_kernel(n_slab, n_sub, per, child_ref, m2m_ref, partners_ref, win_ref, words_ref, table_ref,
                    block, mine, w_send, w_recv, b_send, b_recv, lo_send, lo_recv, hi_send, hi_recv, own_sem):
    slab = lax.axis_index("slab")
    sub = lax.axis_index("sub")
    lower = (slab + n_slab - 1) % n_slab
    upper = (slab + 1) % n_slab
    steps = peers_of(sub, n_sub)
    cells = block.shape[1]

    barrier = pltpu.get_barrier_semaphore()
    for step in steps:
        pl.semaphore_signal(barrier, inc=1, device_id={"slab": slab, "sub": moved(sub, step, 1)}, device_id_type=MESH)
    for other in (lower, upper):
        pl.semaphore_signal(barrier, inc=1, device_id={"slab": other, "sub": sub}, device_id_type=MESH)

    base = (slab - 1) * (n_sub * cells)
    lane = lax.broadcasted_iota(jnp.int32, (per, cells), 1)
    for j in range(n_sub):
        p = partners_ref[per * j : per * (j + 1), :]
        rel = p - base
        brick = jnp.where(p >= 0, jnp.right_shift(rel, 7), NONE)
        code = jnp.full(p.shape, 512, jnp.int32)
        packed = jnp.zeros(p.shape, jnp.int32)
        last = jnp.full((per, 1), -1, jnp.int32)
        for c in range(4):
            last = jnp.min(jnp.where(brick > last, brick, NONE), axis=1, keepdims=True)
            code = jnp.where((brick == last) & (brick < NONE), c * 128 + jnp.bitwise_and(rel, 127), code)
            packed = jnp.where(lane % 4 == c, jnp.where(last < NONE, last, n_sub), packed)
        mine[j, 0:per, :] = code + packed * 1024
        mine[j, per:16, :] = jnp.full((16 - per, cells), 512, jnp.int32)

    diff = lax.broadcasted_iota(jnp.int32, (8 * cells, cells), 0) - 8 * lax.broadcasted_iota(jnp.int32, (8 * cells, cells), 1)
    children = child_ref[...]
    total = jnp.zeros((block.shape[0], cells), F32)
    for o in range(8):
        pick = jnp.where(diff == o, 1.0, 0.0).astype(BF16)
        column = jnp.dot(children, pick, preferred_element_type=F32).astype(BF16)
        total += jnp.dot(m2m_ref[o], column, preferred_element_type=F32)
    block[...] = total.astype(BF16)

    pl.semaphore_wait(barrier, len(steps) + 2)

    copies = []

    def send(src, dst, send_sem, recv_sem, device):
        copy = pltpu.make_async_remote_copy(
            src_ref=src, dst_ref=dst, send_sem=send_sem, recv_sem=recv_sem, device_id=device, device_id_type=MESH
        )
        copy.start()
        copies.append(copy)

    own = pltpu.make_async_copy(block, win_ref.at[n_sub + sub], own_sem.at[0])
    own.start()
    own_words = pltpu.make_async_copy(mine.at[sub], words_ref.at[sub], own_sem.at[1])
    own_words.start()
    for d, step in enumerate(steps):
        to = moved(sub, step, 1)
        send(block, win_ref.at[n_sub + sub], b_send.at[d], b_recv.at[d], {"slab": slab, "sub": to})
        if d == 0:
            send(block, win_ref.at[2 * n_sub + sub], lo_send.at[15], lo_recv.at[15], {"slab": lower, "sub": sub})
            send(block, win_ref.at[sub], hi_send.at[15], hi_recv.at[15], {"slab": upper, "sub": sub})
    for d, step in enumerate(steps):
        to = moved(sub, step, 1)
        send(mine.at[to], words_ref.at[sub], w_send.at[d], w_recv.at[d], {"slab": slab, "sub": to})
    for d, step in enumerate(steps):
        origin = moved(sub, step, -1)
        arrived = pltpu.make_async_remote_copy(
            src_ref=block, dst_ref=win_ref.at[n_sub + origin], send_sem=b_send.at[d], recv_sem=b_recv.at[d],
            device_id={"slab": slab, "sub": origin}, device_id_type=MESH,
        )
        arrived.wait_recv()
        place = win_ref.at[n_sub + origin]
        send(place, win_ref.at[2 * n_sub + origin], lo_send.at[d], lo_recv.at[d], {"slab": lower, "sub": sub})
        send(place, win_ref.at[origin], hi_send.at[d], hi_recv.at[d], {"slab": upper, "sub": sub})
    own.wait()
    own_words.wait()
    for d, step in enumerate(steps):
        origin = moved(sub, step, -1)
        pltpu.make_async_remote_copy(
            src_ref=mine.at[0], dst_ref=words_ref.at[origin], send_sem=w_send.at[d], recv_sem=w_recv.at[d],
            device_id={"slab": slab, "sub": origin}, device_id_type=MESH,
        ).wait_recv()
    flat = jnp.concatenate([words_ref[j] for j in range(n_sub)], axis=0)
    table_ref[...] = jnp.right_shift(jnp.transpose(flat)[0:8, :], 10)
    for d in range(16):
        origin = sub if d == 15 else moved(sub, steps[d], -1)
        pltpu.make_async_remote_copy(
            src_ref=block, dst_ref=win_ref.at[2 * n_sub + origin], send_sem=lo_send.at[d], recv_sem=lo_recv.at[d],
            device_id={"slab": upper, "sub": sub}, device_id_type=MESH,
        ).wait_recv()
        pltpu.make_async_remote_copy(
            src_ref=block, dst_ref=win_ref.at[origin], send_sem=hi_send.at[d], recv_sem=hi_recv.at[d],
            device_id={"slab": lower, "sub": sub}, device_id_type=MESH,
        ).wait_recv()
    for copy in copies:
        copy.wait_send()


def transfer_kernel(per, table_ref, win_ref, words_ref, ops_ref, part_ref):
    rows, cells = part_ref.shape[1:]

    def brick(b, carry):
        total = jnp.zeros((rows, cells), F32)
        for k in range(per):
            code = jnp.bitwise_and(words_ref[b][k : k + 1, :], 1023)
            place = jnp.broadcast_to(jnp.bitwise_and(code, 127), (rows, cells))
            which = jnp.right_shift(code, 7)
            columns = jnp.zeros((rows, cells), F32)
            for c in range(4):
                source = win_ref[table_ref[c, b * 16 + k]].astype(F32)
                got = jnp.take_along_axis(source, place, axis=1, mode="promise_in_bounds")
                columns = jnp.where(which == c, got, columns)
            total += jnp.dot(ops_ref[k], columns.astype(BF16), preferred_element_type=F32)
        part_ref[b] = total.astype(BF16)
        return carry

    lax.fori_loop(0, part_ref.shape[0], brick, 0)


def finish_kernel(n_sub, part_ref, incoming_ref, l2l_ref, out_ref, got, p_send, p_recv):
    slab = lax.axis_index("slab")
    sub = lax.axis_index("sub")
    steps = peers_of(sub, n_sub)
    cells = incoming_ref.shape[1]
    barrier = pltpu.get_barrier_semaphore()
    for step in steps:
        pl.semaphore_signal(barrier, inc=1, device_id={"slab": slab, "sub": moved(sub, step, 1)}, device_id_type=MESH)
    pl.semaphore_wait(barrier, len(steps))
    copies = []
    for d, step in enumerate(steps):
        to = moved(sub, step, 1)
        copy = pltpu.make_async_remote_copy(
            src_ref=part_ref.at[to], dst_ref=got.at[d], send_sem=p_send.at[d], recv_sem=p_recv.at[d],
            device_id={"slab": slab, "sub": to}, device_id_type=MESH,
        )
        copy.start()
        copies.append(copy)
    total = part_ref[sub].astype(F32)
    for d, copy in enumerate(copies):
        copy.wait_recv()
        total += got[d].astype(F32)
    local = (incoming_ref[...].astype(F32) + total).astype(BF16)
    wide = 256
    for g in range(8 * cells // wide):
        row = lax.broadcasted_iota(jnp.int32, (cells, wide), 0)
        column = lax.broadcasted_iota(jnp.int32, (cells, wide), 1) + g * wide
        spread = jnp.where(jnp.right_shift(column, 3) == row, 1.0, 0.0).astype(BF16)
        repeated = jnp.dot(local, spread, preferred_element_type=F32)
        octant = jnp.bitwise_and(lax.broadcasted_iota(jnp.int32, repeated.shape, 1), 7)
        result = jnp.zeros(repeated.shape, F32)
        for o in range(8):
            kept = jnp.where(octant == o, repeated, 0.0).astype(BF16)
            result += jnp.dot(l2l_ref[o], kept, preferred_element_type=F32)
        out_ref[:, g * wide : (g + 1) * wide] = result
    for copy in copies:
        copy.wait_send()


def solution(mesh):
    n_slab, n_sub = mesh.shape["slab"], mesh.shape["sub"]
    dma = pltpu.SemaphoreType.DMA

    def local(child_moments, incoming, m2m_ops, m2l_ops, l2l_ops, partners):
        rows = child_moments.shape[0]
        cells = incoming.shape[1]
        per = m2l_ops.shape[0]
        win, words, table = pl.pallas_call(
            functools.partial(exchange_kernel, n_slab, n_sub, per),
            name="exchange",
            out_shape=(
                jax.ShapeDtypeStruct((3 * n_sub, rows, cells), BF16),
                jax.ShapeDtypeStruct((n_sub, 16, cells), jnp.int32),
                jax.ShapeDtypeStruct((8, n_sub * 16), jnp.int32),
            ),
            in_specs=[VM] * 3,
            out_specs=(VM, VM, VM),
            scratch_shapes=[
                pltpu.VMEM((rows, cells), BF16),
                pltpu.VMEM((n_sub, 16, cells), jnp.int32),
            ]
            + [dma((16,))] * 8
            + [dma((2,))],
            compiler_params=pltpu.CompilerParams(collective_id=0, has_side_effects=True, vmem_limit_bytes=24 * 2**20),
        )(child_moments, m2m_ops, partners)
        part = pl.pallas_call(
            functools.partial(transfer_kernel, per),
            name="transfer",
            out_shape=jax.ShapeDtypeStruct((n_sub, rows, cells), BF16),
            in_specs=[pl.BlockSpec(memory_space=pltpu.SMEM)] + [VM] * 3,
            out_specs=VM,
            compiler_params=pltpu.CompilerParams(vmem_limit_bytes=24 * 2**20),
        )(table, win, words, m2l_ops)
        return pl.pallas_call(
            functools.partial(finish_kernel, n_sub),
            name="finish",
            out_shape=jax.ShapeDtypeStruct((rows, 8 * cells), F32),
            in_specs=[VM] * 3,
            out_specs=VM,
            scratch_shapes=[pltpu.VMEM((n_sub - 1, rows, cells), BF16), dma((16,)), dma((16,))],
            compiler_params=pltpu.CompilerParams(collective_id=1, has_side_effects=True, vmem_limit_bytes=24 * 2**20),
        )(part, incoming, l2l_ops)

    in_specs = (
        P(None, ("slab", "sub")),
        P(None, ("slab", "sub")),
        P(),
        P("sub", None, None),
        P(),
        P(None, ("slab", "sub")),
    )
    return jax.shard_map(local, mesh=mesh, in_specs=in_specs, out_specs=P(None, ("slab", "sub")), check_vma=False)
```

```python
import functools

import jax
import jax.numpy as jnp
from jax import lax
from jax.experimental import pallas as pl
from jax.experimental.pallas import tpu as pltpu
from jax.sharding import PartitionSpec as P

MESH = pl.DeviceIdType.MESH
F32 = jnp.float32
BF16 = jnp.bfloat16
VM = pl.BlockSpec(memory_space=pltpu.VMEM)
HB = pl.BlockSpec(memory_space=pltpu.HBM)
NONE = 64


def hops(i):
    return min(i // 4, 4 - i // 4) + min(i % 4, 4 - i % 4)


ORDER = sorted(range(1, 16), key=hops)


def moved(sub, i, sign):
    x, y = sub // 4, sub % 4
    return (x + sign * (i // 4) + 4) % 4 * 4 + (y + sign * (i % 4) + 4) % 4


def main_kernel(n_slab, n_sub, per, child_hbm, incoming_hbm, m2m_hbm, ops_hbm, partners_hbm, local_ref,
                child_ref, incoming_ref, m2m_ref, ops_ref, partners_ref, in_sem,
                block, win_ref, mine, words_ref, table_ref, table_smem, part_ref, got,
                w_send, w_recv, b_send, b_recv, lo_send, lo_recv, hi_send, hi_recv, p_send, p_recv, own_sem):
    slab = lax.axis_index("slab")
    sub = lax.axis_index("sub")
    lower = (slab + n_slab - 1) % n_slab
    upper = (slab + 1) % n_slab
    rows, cells = block.shape

    loads = [
        pltpu.make_async_copy(source, target, in_sem.at[i])
        for i, (source, target) in enumerate(
            [(partners_hbm, partners_ref), (child_hbm, child_ref), (m2m_hbm, m2m_ref), (ops_hbm, ops_ref), (incoming_hbm, incoming_ref)]
        )
    ]
    for load in loads:
        load.start()
    barrier = pltpu.get_barrier_semaphore()
    for i in range(1, n_sub):
        pl.semaphore_signal(barrier, inc=1, device_id={"slab": slab, "sub": moved(sub, i, 1)}, device_id_type=MESH)
    for other in (lower, upper):
        pl.semaphore_signal(barrier, inc=1, device_id={"slab": other, "sub": sub}, device_id_type=MESH)

    diff = lax.broadcasted_iota(jnp.int32, (8 * cells, cells), 0) - 8 * lax.broadcasted_iota(jnp.int32, (8 * cells, cells), 1)
    loads[1].wait()
    children = child_ref[...]
    columns = []
    for o in range(0, 8, 2):
        pick = jnp.concatenate([jnp.where(diff == q, 1.0, 0.0).astype(BF16) for q in (o, o + 1)], axis=1)
        both = jnp.dot(children, pick, preferred_element_type=F32).astype(BF16)
        columns += [both[:, :cells], both[:, cells:]]
    loads[2].wait()
    total = jnp.zeros((rows, cells), F32)
    for o in range(8):
        total += jnp.dot(m2m_ref[o], columns[o], preferred_element_type=F32)
    moments = total.astype(BF16)
    block[...] = moments
    win_ref[n_sub + sub] = moments
    pl.semaphore_wait(barrier, n_sub + 1)

    copies = []

    def send(src, dst, send_sem, recv_sem, device):
        copy = pltpu.make_async_remote_copy(
            src_ref=src, dst_ref=dst, send_sem=send_sem, recv_sem=recv_sem, device_id=device, device_id_type=MESH
        )
        copy.start()
        copies.append(copy)

    def expect(dst, send_sem, recv_sem, device):
        pltpu.make_async_remote_copy(
            src_ref=dst, dst_ref=dst, send_sem=send_sem, recv_sem=recv_sem, device_id=device, device_id_type=MESH
        ).wait_recv()

    for i in ORDER:
        if i == ORDER[4]:
            send(block, win_ref.at[2 * n_sub + sub], lo_send.at[0], lo_recv.at[0], {"slab": lower, "sub": sub})
            send(block, win_ref.at[sub], hi_send.at[0], hi_recv.at[0], {"slab": upper, "sub": sub})
        send(block, win_ref.at[n_sub + sub], b_send.at[i], b_recv.at[i], {"slab": slab, "sub": moved(sub, i, 1)})

    loads[0].wait()
    base = (slab - 1) * (n_sub * cells)
    lane = lax.broadcasted_iota(jnp.int32, (per, cells), 1)
    place = lax.broadcasted_iota(jnp.int32, (cells, cells), 0)
    across = lax.broadcasted_iota(jnp.int32, (cells, cells), 1)

    def words_for(group):
        codes, tables, which_of = [], [], []
        for j in range(8 * group, 8 * group + 8):
            p = partners_ref[per * j : per * (j + 1), :]
            rel = p - base
            brick = jnp.where(p >= 0, jnp.right_shift(rel, 7), NONE)
            which = jnp.zeros(p.shape, jnp.int32)
            packed = jnp.zeros(p.shape, jnp.int32)
            last = jnp.full((per, 1), -1, jnp.int32)
            for c in range(4):
                last = jnp.min(jnp.where(brick > last, brick, NONE), axis=1, keepdims=True)
                which = jnp.where((brick == last) & (brick < NONE), c, which)
                packed = jnp.where(lane % 4 == c, jnp.where(last < NONE, last, n_sub), packed)
            codes.append(jnp.where(p >= 0, jnp.bitwise_and(rel, 127) + 128, 0))
            tables.append(packed)
            which_of.append(which.astype(F32))
            which_of.append(jnp.zeros((16 - per, cells), F32))
        turned = jnp.transpose(jnp.concatenate(which_of, axis=0))
        back = jnp.zeros((cells, cells), F32)
        for j in range(8):
            left, right = [], []
            for k in range(per):
                left.append(jnp.where(jnp.bitwise_and(codes[j][k : k + 1, :], 127) == place, 1.0, 0.0).astype(BF16))
                right.append(jnp.where(across == 16 * j + k, turned, 0.0).astype(BF16))
            back += jnp.dot(jnp.concatenate(left, axis=1), jnp.concatenate(right, axis=0), preferred_element_type=F32)
        back = jnp.transpose(back).astype(jnp.int32)
        for j in range(8):
            mine[8 * group + j, 0:per, :] = codes[j] + jnp.bitwise_and(back[16 * j : 16 * j + per, :], 3) * 256 + tables[j] * 1024
            mine[8 * group + j, per:16, :] = jnp.zeros((16 - per, cells), jnp.int32)

    words_for(0)
    for n, i in enumerate(ORDER):
        origin = moved(sub, i, -1)
        expect(win_ref.at[n_sub + origin], b_send.at[i], b_recv.at[i], {"slab": slab, "sub": origin})
        source = win_ref.at[n_sub + origin]
        send(source, win_ref.at[2 * n_sub + origin], lo_send.at[i], lo_recv.at[i], {"slab": lower, "sub": sub})
        send(source, win_ref.at[origin], hi_send.at[i], hi_recv.at[i], {"slab": upper, "sub": sub})
        if n == 5:
            words_for(1)
    for i in ORDER:
        to = moved(sub, i, 1)
        send(mine.at[to], words_ref.at[sub], w_send.at[i], w_recv.at[i], {"slab": slab, "sub": to})
    words_ref[sub] = mine[sub]
    for i in ORDER:
        origin = moved(sub, i, -1)
        expect(words_ref.at[origin], w_send.at[i], w_recv.at[i], {"slab": slab, "sub": origin})
    flat = jnp.concatenate([words_ref[j] for j in range(n_sub)], axis=0)
    table_ref[...] = jnp.minimum(jnp.bitwise_and(jnp.right_shift(jnp.transpose(flat)[0:8, :], 10), 63), 3 * n_sub - 1)
    to_smem = pltpu.make_async_copy(table_ref, table_smem, own_sem.at[0])
    to_smem.start()
    loads[3].wait()
    to_smem.wait()
    for i in [0] + ORDER:
        origin = moved(sub, i, -1)
        expect(win_ref.at[2 * n_sub + origin], lo_send.at[i], lo_recv.at[i], {"slab": upper, "sub": sub})
        expect(win_ref.at[origin], hi_send.at[i], hi_recv.at[i], {"slab": lower, "sub": sub})

    def columns_of(b, k):
        word = words_ref[b][k : k + 1, :]
        local = jnp.broadcast_to(jnp.bitwise_and(word, 127), (rows, cells))
        which = jnp.broadcast_to(jnp.bitwise_and(jnp.right_shift(word, 8), 3), (rows, cells)).astype(jnp.int16)
        there = jnp.broadcast_to(jnp.bitwise_and(word, 128), (rows, cells)).astype(jnp.int16)
        merged = win_ref[table_smem[0, b * 16 + k]]
        for c in range(1, 4):
            merged = jnp.where(which == c, win_ref[table_smem[c, b * 16 + k]], merged)
        got = jnp.take_along_axis(merged.astype(F32), local, axis=1, mode="promise_in_bounds").astype(BF16)
        return jnp.where(there != 0, got, jnp.zeros((), BF16))

    def part_copy(i, target):
        return pltpu.make_async_remote_copy(
            src_ref=part_ref.at[i], dst_ref=got.at[i], send_sem=p_send.at[i], recv_sem=p_recv.at[i],
            device_id={"slab": slab, "sub": target}, device_id_type=MESH,
        )

    def two_bricks(n, carry):
        ids = [15 - 2 * n, 14 - 2 * n]
        bricks = [moved(sub, i, 1) for i in ids]
        total = jnp.zeros((rows, 2 * cells), F32)
        for k in range(per):
            both = jnp.concatenate([columns_of(b, k) for b in bricks], axis=1)
            total += jnp.dot(ops_ref[k], both, preferred_element_type=F32)
        for q, (i, b) in enumerate(zip(ids, bricks)):
            part_ref[i] = total[:, q * cells : (q + 1) * cells].astype(BF16)

            @pl.when(i != 0)
            def _():
                part_copy(i, b).start()

        return carry

    lax.fori_loop(0, n_sub // 2, two_bricks, 0)
    loads[4].wait()
    total = part_ref[0].astype(F32)
    for i in reversed(ORDER):
        part_copy(i, moved(sub, i, -1)).wait_recv()
        total += got[i].astype(F32)
    local_ref[...] = (incoming_ref[...].astype(F32) + total).astype(BF16)
    for i in ORDER:
        part_copy(i, moved(sub, i, 1)).wait_send()
    for copy in copies:
        copy.wait_send()


def children_kernel(local_ref, l2l_ref, out_ref):
    rows, wide = out_ref.shape
    cells = local_ref.shape[1]
    row = lax.broadcasted_iota(jnp.int32, (cells, wide), 0)
    column = lax.broadcasted_iota(jnp.int32, (cells, wide), 1) + pl.program_id(0) * wide
    spread = jnp.where(jnp.right_shift(column, 3) == row, 1.0, 0.0).astype(BF16)
    repeated = jnp.dot(local_ref[...], spread, preferred_element_type=F32)
    octant = jnp.bitwise_and(lax.broadcasted_iota(jnp.int32, repeated.shape, 1), 7)
    result = jnp.zeros(repeated.shape, F32)
    for o in range(8):
        kept = jnp.where(octant == o, repeated, 0.0).astype(BF16)
        result += jnp.dot(l2l_ref[o], kept, preferred_element_type=F32)
    out_ref[...] = result


def solution(mesh):
    n_slab, n_sub = mesh.shape["slab"], mesh.shape["sub"]
    dma = pltpu.SemaphoreType.DMA

    def local(child_moments, incoming, m2m_ops, m2l_ops, l2l_ops, partners):
        rows = child_moments.shape[0]
        cells = incoming.shape[1]
        per = m2l_ops.shape[0]
        locals_all = pl.pallas_call(
            functools.partial(main_kernel, n_slab, n_sub, per),
            name="main",
            out_shape=jax.ShapeDtypeStruct((rows, cells), BF16),
            in_specs=[HB] * 5,
            out_specs=VM,
            scratch_shapes=[pltpu.VMEM(a.shape, a.dtype) for a in (child_moments, incoming, m2m_ops, m2l_ops, partners)]
            + [
                dma((5,)),
                pltpu.VMEM((rows, cells), BF16),
                pltpu.VMEM((3 * n_sub, rows, cells), BF16),
                pltpu.VMEM((n_sub, 16, cells), jnp.int32),
                pltpu.VMEM((n_sub, 16, cells), jnp.int32),
                pltpu.VMEM((8, n_sub * 16), jnp.int32),
                pltpu.SMEM((8, n_sub * 16), jnp.int32),
                pltpu.VMEM((n_sub, rows, cells), BF16),
                pltpu.VMEM((n_sub, rows, cells), BF16),
            ]
            + [dma((16,))] * 10
            + [dma((1,))],
            compiler_params=pltpu.CompilerParams(collective_id=0, has_side_effects=True, vmem_limit_bytes=66_200_000),
        )(child_moments, incoming, m2m_ops, m2l_ops, partners)
        wide = 256
        return pl.pallas_call(
            children_kernel,
            name="children",
            out_shape=jax.ShapeDtypeStruct((rows, 8 * cells), F32),
            grid=(8 * cells // wide,),
            in_specs=[VM, VM],
            out_specs=pl.BlockSpec((rows, wide), lambda g: (0, g)),
            compiler_params=pltpu.CompilerParams(vmem_limit_bytes=16 * 2**20),
        )(locals_all, l2l_ops)

    in_specs = (
        P(None, ("slab", "sub")),
        P(None, ("slab", "sub")),
        P(),
        P("sub", None, None),
        P(),
        P(None, ("slab", "sub")),
    )
    return jax.shard_map(local, mesh=mesh, in_specs=in_specs, out_specs=P(None, ("slab", "sub")), check_vma=False)
```

```python
import functools

import jax
import jax.numpy as jnp
from jax import lax
from jax.experimental import pallas as pl
from jax.experimental.pallas import tpu as pltpu
from jax.sharding import PartitionSpec as P

MESH = pl.DeviceIdType.MESH
F32 = jnp.float32
BF16 = jnp.bfloat16
VM = pl.BlockSpec(memory_space=pltpu.VMEM)
HB = pl.BlockSpec(memory_space=pltpu.HBM)
NONE = 64
LIMIT = 66_200_000


ORDER = [0, 4, 12, 1, 3, 8, 2, 5, 7, 13, 15, 9, 11, 6, 14, 10]
GROUPS = [(0, 1), (1, 3), (3, 5), (5, 7), (7, 9), (9, 11), (11, 13), (13, 15), (15, 16)]
AXES = ORDER[1:7]
SPLIT = 112


def moved(sub, i, sign):
    x, y = sub // 4, sub % 4
    return (x + sign * (i // 4) + 4) % 4 * 4 + (y + sign * (i % 4) + 4) % 4


def main_kernel(n_slab, n_sub, per, child_hbm, incoming_hbm, m2m_hbm, ops_hbm, l2l_hbm, partners_hbm, out_hbm,
                child_ref, incoming_ref, m2m_ref, ops_ref, l2l_ref, partners_ref, in_sem,
                block, win_ref, mine, words_ref, table_ref, table_smem, part_ref, got,
                w_send, w_recv, b_send, b_recv, h_send, h_recv, lo_send, lo_recv, hi_send, hi_recv, p_send, p_recv, own_sem, result_ref, out_sem):
    slab = lax.axis_index("slab")
    sub = lax.axis_index("sub")
    lower = (slab + n_slab - 1) % n_slab
    upper = (slab + 1) % n_slab
    rows, cells = block.shape

    loads = [
        pltpu.make_async_copy(source, target, in_sem.at[i])
        for i, (source, target) in enumerate(
            [(child_hbm, child_ref), (m2m_hbm, m2m_ref), (partners_hbm, partners_ref), (ops_hbm, ops_ref), (incoming_hbm, incoming_ref), (l2l_hbm, l2l_ref)]
        )
    ]
    for load in loads:
        load.start()
    barrier = pltpu.get_barrier_semaphore()
    for i in range(1, n_sub):
        pl.semaphore_signal(barrier, inc=1, device_id={"slab": slab, "sub": moved(sub, i, 1)}, device_id_type=MESH)
    for other in (lower, upper):
        pl.semaphore_signal(barrier, inc=1, device_id={"slab": other, "sub": sub}, device_id_type=MESH)

    source = lax.broadcasted_iota(jnp.int32, (256, 256), 0)
    lane = lax.broadcasted_iota(jnp.int32, (256, 256), 1)
    picks = []
    for h in range(4):
        o = jnp.bitwise_and(jnp.right_shift(lane, 5) - h, 3) + jnp.bitwise_and(jnp.right_shift(lane, 5), 4)
        picks.append(jnp.where(source == 8 * jnp.bitwise_and(lane, 31) + o, 1.0, 0.0).astype(BF16))
    loads[0].wait()
    spread = [jnp.dot(child_ref[:, 256 * h : 256 * (h + 1)], picks[h], preferred_element_type=F32).astype(BF16) for h in range(4)]
    loads[1].wait()
    quarter = lax.broadcasted_iota(jnp.int32, (rows, cells), 1) // 32
    total = jnp.zeros((rows, cells), F32)
    for r in range(4):
        turned = jnp.zeros((rows, cells), F32)
        for o in (r, r + 4):
            half = [piece[:, cells * (o // 4) : cells * (o // 4 + 1)].astype(F32) for piece in spread]
            column = half[(0 - r) % 4]
            for q in range(1, 4):
                column = jnp.where(quarter == q, half[(q - r) % 4], column)
            turned += jnp.dot(m2m_ref[o], column.astype(BF16), preferred_element_type=F32)
        total += turned if r == 0 else pltpu.roll(turned, cells - 32 * r, 1)
    moments = total.astype(BF16)
    block[...] = moments
    win_ref[n_sub] = moments
    pl.semaphore_wait(barrier, n_sub + 1)

    copies = []

    def send(src, dst, send_sem, recv_sem, device):
        copy = pltpu.make_async_remote_copy(
            src_ref=src, dst_ref=dst, send_sem=send_sem, recv_sem=recv_sem, device_id=device, device_id_type=MESH
        )
        copy.start()
        copies.append(copy)

    def expect(dst, send_sem, recv_sem, device):
        pltpu.make_async_remote_copy(
            src_ref=dst, dst_ref=dst, send_sem=send_sem, recv_sem=recv_sem, device_id=device, device_id_type=MESH
        ).wait_recv()

    def beside(first, last):
        for device, place, sends, recvs in ((lower, 2 * n_sub, lo_send, lo_recv), (upper, 0, hi_send, hi_recv)):
            send(
                win_ref.at[n_sub + first : n_sub + last],
                win_ref.at[place + first : place + last], sends.at[first], recvs.at[first], {"slab": device, "sub": sub},
            )

    beside(0, 1)
    for i in AXES:
        send(block, win_ref.at[n_sub + ORDER.index(i)], b_send.at[i], b_recv.at[i], {"slab": slab, "sub": moved(sub, i, 1)})
    halves = (pl.ds(0, SPLIT), pl.ds(SPLIT, rows - SPLIT))

    loads[2].wait()
    base = (slab - 1) * (n_sub * cells)
    lane = lax.broadcasted_iota(jnp.int32, (per, cells), 1)
    place = lax.broadcasted_iota(jnp.int32, (cells, cells), 0)
    across = lax.broadcasted_iota(jnp.int32, (cells, cells), 1)

    def words_for(group):
        codes, tables, which_of = [], [], []
        for j in range(8 * group, 8 * group + 8):
            p = partners_ref[per * j : per * (j + 1), :]
            rel = p - base
            brick = jnp.where(p >= 0, jnp.right_shift(rel, 7), NONE)
            which = jnp.zeros(p.shape, jnp.int32)
            packed = jnp.zeros(p.shape, jnp.int32)
            last = jnp.full((per, 1), -1, jnp.int32)
            for c in range(4):
                last = jnp.min(jnp.where(brick > last, brick, NONE), axis=1, keepdims=True)
                which = jnp.where((brick == last) & (brick < NONE), c, which)
                packed = jnp.where(lane % 4 == c, jnp.where(last < NONE, last, n_sub), packed)
            codes.append(jnp.where(p >= 0, jnp.bitwise_and(rel, 127) + 128, 0))
            tables.append(packed)
            which_of.append(which.astype(F32))
            which_of.append(jnp.zeros((16 - per, cells), F32))
        turned = jnp.transpose(jnp.concatenate(which_of, axis=0))
        back = jnp.zeros((cells, cells), F32)
        for j in range(8):
            left, right = [], []
            for k in range(per):
                left.append(jnp.where(jnp.bitwise_and(codes[j][k : k + 1, :], 127) == place, 1.0, 0.0).astype(BF16))
                right.append(jnp.where(across == 16 * j + k, turned, 0.0).astype(BF16))
            back += jnp.dot(jnp.concatenate(left, axis=1), jnp.concatenate(right, axis=0), preferred_element_type=F32)
        back = jnp.transpose(back).astype(jnp.int32)
        for j in range(8):
            mine[8 * group + j, 0:per, :] = codes[j] + jnp.bitwise_and(back[16 * j : 16 * j + per, :], 3) * 256 + tables[j] * 1024
            mine[8 * group + j, per:16, :] = jnp.zeros((16 - per, cells), jnp.int32)

    words_for(0)
    for first, last in GROUPS[1:]:
        for n in range(first, last):
            i = ORDER[n]
            origin = {"slab": slab, "sub": moved(sub, i, -1)}
            landed = win_ref.at[n_sub + n]
            if i in AXES:
                expect(landed, b_send.at[i], b_recv.at[i], origin)
                half, onward = (0, (1, 3, 2)) if i % 4 == 0 else (1, (4, 12, 8))
                for step in onward:
                    m = ORDER.index(i + step)
                    send(
                        landed.at[halves[half]], win_ref.at[n_sub + m, halves[half]], h_send.at[half, i + step], h_recv.at[half, i + step],
                        {"slab": slab, "sub": moved(sub, step, 1)},
                    )
            else:
                for half in range(2):
                    expect(landed.at[halves[half]], h_send.at[half, i], h_recv.at[half, i], origin)
        beside(first, last)
        if last == 7:
            words_for(1)
            for i in reversed(ORDER[1:]):
                to = moved(sub, i, 1)
                send(mine.at[to], words_ref.at[sub], w_send.at[i], w_recv.at[i], {"slab": slab, "sub": to})
            words_ref[sub] = mine[sub]
    for i in ORDER[1:]:
        origin = moved(sub, i, -1)
        expect(words_ref.at[origin], w_send.at[i], w_recv.at[i], {"slab": slab, "sub": origin})
    flat = jnp.concatenate([words_ref[j] for j in range(n_sub)], axis=0)
    brick = jnp.bitwise_and(jnp.right_shift(jnp.transpose(flat)[0:8, :], 10), 63)
    offset = jnp.bitwise_and(sub // 4 - jnp.right_shift(brick, 2), 3) * 4 + jnp.bitwise_and(sub - brick, 3)
    slot = jnp.zeros(brick.shape, jnp.int32)
    for n, i in enumerate(ORDER):
        slot = jnp.where(offset == i, n, slot)
    table_ref[...] = jnp.minimum(jnp.bitwise_and(brick, 48), 2 * n_sub) + slot
    to_smem = pltpu.make_async_copy(table_ref, table_smem, own_sem.at[0])
    to_smem.start()
    loads[3].wait()
    to_smem.wait()
    for first, last in GROUPS:
        expect(win_ref.at[2 * n_sub + first : 2 * n_sub + last], lo_send.at[first], lo_recv.at[first], {"slab": upper, "sub": sub})
        expect(win_ref.at[first:last], hi_send.at[first], hi_recv.at[first], {"slab": lower, "sub": sub})

    def columns_of(b, k):
        word = words_ref[b][k : k + 1, :]
        local = jnp.broadcast_to(jnp.bitwise_and(word, 127), (rows, cells))
        which = jnp.broadcast_to(jnp.bitwise_and(jnp.right_shift(word, 8), 3), (rows, cells)).astype(jnp.int16)
        there = jnp.broadcast_to(jnp.bitwise_and(word, 128), (rows, cells)).astype(jnp.int16)
        merged = win_ref[table_smem[0, b * 16 + k]]
        for c in range(1, 4):
            merged = jnp.where(which == c, win_ref[table_smem[c, b * 16 + k]], merged)
        got = jnp.take_along_axis(merged.astype(F32), local, axis=1, mode="promise_in_bounds").astype(BF16)
        return jnp.where(there != 0, got, jnp.zeros((), BF16))

    def part_copy(i, target):
        return pltpu.make_async_remote_copy(
            src_ref=part_ref.at[i], dst_ref=got.at[i], send_sem=p_send.at[i], recv_sem=p_recv.at[i],
            device_id={"slab": slab, "sub": target}, device_id_type=MESH,
        )

    def two_bricks(n, carry):
        ids = [15 - 2 * n, 14 - 2 * n]
        bricks = [moved(sub, i, 1) for i in ids]
        total = jnp.zeros((rows, 2 * cells), F32)
        for k in range(per):
            both = jnp.concatenate([columns_of(b, k) for b in bricks], axis=1)
            total += jnp.dot(ops_ref[k], both, preferred_element_type=F32)
        for q, (i, b) in enumerate(zip(ids, bricks)):
            part_ref[i] = total[:, q * cells : (q + 1) * cells].astype(BF16)

            @pl.when(i != 0)
            def _():
                part_copy(i, b).start()

        return carry

    lax.fori_loop(0, n_sub // 2, two_bricks, 0)
    loads[4].wait()
    total = part_ref[0].astype(F32)
    for i in reversed(ORDER[1:]):
        part_copy(i, moved(sub, i, -1)).wait_recv()
        total += got[i].astype(F32)
    locals_all = (incoming_ref[...].astype(F32) + total).astype(BF16)
    loads[5].wait()
    wide = 2 * cells
    stores = []
    for g in range(8 * cells // wide):
        row = lax.broadcasted_iota(jnp.int32, (cells, wide), 0)
        column = lax.broadcasted_iota(jnp.int32, (cells, wide), 1) + g * wide
        spread = jnp.where(jnp.right_shift(column, 3) == row, 1.0, 0.0).astype(BF16)
        repeated = jnp.dot(locals_all, spread, preferred_element_type=F32)
        octant = jnp.bitwise_and(lax.broadcasted_iota(jnp.int32, repeated.shape, 1), 7)
        result = jnp.zeros(repeated.shape, F32)
        for o in range(8):
            kept = jnp.where(octant == o, repeated, 0.0).astype(BF16)
            result += jnp.dot(l2l_ref[o], kept, preferred_element_type=F32)
        result_ref[:, g * wide : (g + 1) * wide] = result
        columns = pl.ds(g * wide, wide)
        stores.append(pltpu.make_async_copy(result_ref.at[:, columns], out_hbm.at[:, columns], out_sem.at[g]))
        stores[-1].start()
    for store in stores:
        store.wait()
    for i in ORDER[1:]:
        part_copy(i, moved(sub, i, 1)).wait_send()
    for copy in copies:
        copy.wait_send()


def solution(mesh):
    n_slab, n_sub = mesh.shape["slab"], mesh.shape["sub"]
    dma = pltpu.SemaphoreType.DMA

    def local(child_moments, incoming, m2m_ops, m2l_ops, l2l_ops, partners):
        rows = child_moments.shape[0]
        cells = incoming.shape[1]
        per = m2l_ops.shape[0]
        args = (child_moments, incoming, m2m_ops, m2l_ops, l2l_ops, partners)
        return pl.pallas_call(
            functools.partial(main_kernel, n_slab, n_sub, per),
            name="main",
            out_shape=jax.ShapeDtypeStruct((rows, 8 * cells), F32),
            in_specs=[HB] * 6,
            out_specs=HB,
            scratch_shapes=[pltpu.VMEM(a.shape, a.dtype) for a in args]
            + [
                dma((6,)),
                pltpu.VMEM((rows, cells), BF16),
                pltpu.VMEM((3 * n_sub, rows, cells), BF16),
                pltpu.VMEM((n_sub, 16, cells), jnp.int32),
                pltpu.VMEM((n_sub, 16, cells), jnp.int32),
                pltpu.VMEM((8, n_sub * 16), jnp.int32),
                pltpu.SMEM((8, n_sub * 16), jnp.int32),
                pltpu.VMEM((n_sub, rows, cells), BF16),
                pltpu.VMEM((n_sub, rows, cells), BF16),
            ]
            + [dma((16,))] * 4
            + [dma((2, 16))] * 2
            + [dma((16,))] * 6
            + [dma((1,)), pltpu.VMEM((rows, 8 * cells), F32), dma((4,))],
            compiler_params=pltpu.CompilerParams(collective_id=0, has_side_effects=True, vmem_limit_bytes=LIMIT),
        )(*args)

    in_specs = (
        P(None, ("slab", "sub")),
        P(None, ("slab", "sub")),
        P(),
        P("sub", None, None),
        P(),
        P(None, ("slab", "sub")),
    )
    return jax.shard_map(local, mesh=mesh, in_specs=in_specs, out_specs=P(None, ("slab", "sub")), check_vma=False)
```

```python
import functools

import jax
import jax.numpy as jnp
from jax import lax
from jax.experimental import pallas as pl
from jax.experimental.pallas import tpu as pltpu
from jax.sharding import PartitionSpec as P

MESH = pl.DeviceIdType.MESH
F32 = jnp.float32
BF16 = jnp.bfloat16
VM = pl.BlockSpec(memory_space=pltpu.VMEM)
HB = pl.BlockSpec(memory_space=pltpu.HBM)
NONE = 64
LIMIT = 66_200_000


ORDER = [0, 4, 12, 1, 3, 8, 2, 5, 7, 13, 15, 9, 11, 6, 14, 10]
GROUPS = [(0, 1), (1, 3), (3, 5), (5, 7), (7, 9), (9, 11), (11, 13), (13, 15), (15, 16)]
AXES = ORDER[1:7]
SPLIT = 112


def moved(sub, i, sign):
    x, y = sub // 4, sub % 4
    return (x + sign * (i // 4) + 4) % 4 * 4 + (y + sign * (i % 4) + 4) % 4


def main_kernel(n_slab, n_sub, per, child_hbm, incoming_hbm, m2m_hbm, ops_hbm, l2l_hbm, partners_hbm, out_hbm,
                child_ref, incoming_ref, m2m_ref, ops_ref, l2l_ref, partners_ref, in_sem,
                block, win_ref, mine, words_ref, table_ref, table_smem, part_ref, got,
                w_send, w_recv, b_send, b_recv, h_send, h_recv, lo_send, lo_recv, hi_send, hi_recv, p_send, p_recv, own_sem, result_ref, out_sem):
    slab = lax.axis_index("slab")
    sub = lax.axis_index("sub")
    lower = (slab + n_slab - 1) % n_slab
    upper = (slab + 1) % n_slab
    rows, cells = block.shape

    loads = [
        pltpu.make_async_copy(source, target, in_sem.at[i])
        for i, (source, target) in enumerate(
            [(child_hbm, child_ref), (m2m_hbm, m2m_ref), (partners_hbm, partners_ref), (ops_hbm, ops_ref), (incoming_hbm, incoming_ref), (l2l_hbm, l2l_ref)]
        )
    ]
    for load in loads:
        load.start()
    barrier = pltpu.get_barrier_semaphore()
    for i in range(1, n_sub):
        pl.semaphore_signal(barrier, inc=1, device_id={"slab": slab, "sub": moved(sub, i, 1)}, device_id_type=MESH)
    has_lower, has_upper = slab > 0, slab < n_slab - 1
    for has, other in ((has_lower, lower), (has_upper, upper)):

        @pl.when(has)
        def _():
            pl.semaphore_signal(barrier, inc=1, device_id={"slab": other, "sub": sub}, device_id_type=MESH)

    for has, edge in ((has_lower, 0), (has_upper, 2 * n_sub)):

        @pl.when(jnp.logical_not(has))
        def _():
            win_ref[edge : edge + n_sub] = jnp.zeros((n_sub, rows, cells), BF16)

    source = lax.broadcasted_iota(jnp.int32, (256, 256), 0)
    lane = lax.broadcasted_iota(jnp.int32, (256, 256), 1)
    picks = []
    for h in range(4):
        o = jnp.bitwise_and(jnp.right_shift(lane, 5) - h, 3) + jnp.bitwise_and(jnp.right_shift(lane, 5), 4)
        picks.append(jnp.where(source == 8 * jnp.bitwise_and(lane, 31) + o, 1.0, 0.0).astype(BF16))
    loads[0].wait()
    spread = [jnp.dot(child_ref[:, 256 * h : 256 * (h + 1)], picks[h], preferred_element_type=F32).astype(BF16) for h in range(4)]
    loads[1].wait()
    quarter = lax.broadcasted_iota(jnp.int32, (rows, cells), 1) // 32
    total = jnp.zeros((rows, cells), F32)
    for r in range(4):
        turned = jnp.zeros((rows, cells), F32)
        for o in (r, r + 4):
            half = [piece[:, cells * (o // 4) : cells * (o // 4 + 1)].astype(F32) for piece in spread]
            column = half[(0 - r) % 4]
            for q in range(1, 4):
                column = jnp.where(quarter == q, half[(q - r) % 4], column)
            turned += jnp.dot(m2m_ref[o], column.astype(BF16), preferred_element_type=F32)
        total += turned if r == 0 else pltpu.roll(turned, cells - 32 * r, 1)
    moments = total.astype(BF16)
    block[...] = moments
    win_ref[n_sub] = moments
    pl.semaphore_wait(barrier, n_sub - 1 + jnp.minimum(slab, 1) + jnp.minimum(n_slab - 1 - slab, 1))

    copies = []

    def send(src, dst, send_sem, recv_sem, device):
        copy = pltpu.make_async_remote_copy(
            src_ref=src, dst_ref=dst, send_sem=send_sem, recv_sem=recv_sem, device_id=device, device_id_type=MESH
        )
        copy.start()
        copies.append(copy)

    def expect(dst, send_sem, recv_sem, device):
        pltpu.make_async_remote_copy(
            src_ref=dst, dst_ref=dst, send_sem=send_sem, recv_sem=recv_sem, device_id=device, device_id_type=MESH
        ).wait_recv()

    def beside_copies(first, last):
        return [
            (
                has,
                pltpu.make_async_remote_copy(
                    src_ref=win_ref.at[n_sub + first : n_sub + last], dst_ref=win_ref.at[place + first : place + last],
                    send_sem=sends.at[first], recv_sem=recvs.at[first], device_id={"slab": device, "sub": sub}, device_id_type=MESH,
                ),
            )
            for has, device, place, sends, recvs in (
                (has_lower, lower, 2 * n_sub, lo_send, lo_recv), (has_upper, upper, 0, hi_send, hi_recv)
            )
        ]

    def beside(first, last):
        for has, copy in beside_copies(first, last):
            pl.when(has)(copy.start)

    beside(0, 1)
    for i in AXES:
        send(block, win_ref.at[n_sub + ORDER.index(i)], b_send.at[i], b_recv.at[i], {"slab": slab, "sub": moved(sub, i, 1)})
    halves = (pl.ds(0, SPLIT), pl.ds(SPLIT, rows - SPLIT))

    loads[2].wait()
    base = (slab - 1) * (n_sub * cells)
    lane = lax.broadcasted_iota(jnp.int32, (per, cells), 1)
    place = lax.broadcasted_iota(jnp.int32, (cells, cells), 0)
    across = lax.broadcasted_iota(jnp.int32, (cells, cells), 1)

    def words_for(group):
        codes, tables, which_of = [], [], []
        for j in range(8 * group, 8 * group + 8):
            p = partners_ref[per * j : per * (j + 1), :]
            rel = p - base
            brick = jnp.where(p >= 0, jnp.right_shift(rel, 7), NONE)
            which = jnp.zeros(p.shape, jnp.int32)
            packed = jnp.zeros(p.shape, jnp.int32)
            last = jnp.full((per, 1), -1, jnp.int32)
            for c in range(4):
                last = jnp.min(jnp.where(brick > last, brick, NONE), axis=1, keepdims=True)
                which = jnp.where((brick == last) & (brick < NONE), c, which)
                packed = jnp.where(lane % 4 == c, jnp.where(last < NONE, last, n_sub), packed)
            codes.append(jnp.where(p >= 0, jnp.bitwise_and(rel, 127) + 128, 0))
            tables.append(packed)
            which_of.append(which.astype(F32))
            which_of.append(jnp.zeros((16 - per, cells), F32))
        turned = jnp.transpose(jnp.concatenate(which_of, axis=0))
        back = jnp.zeros((cells, cells), F32)
        for j in range(8):
            left, right = [], []
            for k in range(per):
                left.append(jnp.where(jnp.bitwise_and(codes[j][k : k + 1, :], 127) == place, 1.0, 0.0).astype(BF16))
                right.append(jnp.where(across == 16 * j + k, turned, 0.0).astype(BF16))
            back += jnp.dot(jnp.concatenate(left, axis=1), jnp.concatenate(right, axis=0), preferred_element_type=F32)
        back = jnp.transpose(back).astype(jnp.int32)
        for j in range(8):
            mine[8 * group + j, 0:per, :] = codes[j] + jnp.bitwise_and(back[16 * j : 16 * j + per, :], 3) * 256 + tables[j] * 1024
            mine[8 * group + j, per:16, :] = jnp.zeros((16 - per, cells), jnp.int32)

    words_for(0)
    for first, last in GROUPS[1:]:
        for n in range(first, last):
            i = ORDER[n]
            origin = {"slab": slab, "sub": moved(sub, i, -1)}
            landed = win_ref.at[n_sub + n]
            if i in AXES:
                expect(landed, b_send.at[i], b_recv.at[i], origin)
                half, onward = (0, (1, 3, 2)) if i % 4 == 0 else (1, (4, 12, 8))
                for step in onward:
                    m = ORDER.index(i + step)
                    send(
                        landed.at[halves[half]], win_ref.at[n_sub + m, halves[half]], h_send.at[half, i + step], h_recv.at[half, i + step],
                        {"slab": slab, "sub": moved(sub, step, 1)},
                    )
            else:
                for half in range(2):
                    expect(landed.at[halves[half]], h_send.at[half, i], h_recv.at[half, i], origin)
        beside(first, last)
        if last == 7:
            words_for(1)
            for i in reversed(ORDER[1:]):
                to = moved(sub, i, 1)
                send(mine.at[to], words_ref.at[sub], w_send.at[i], w_recv.at[i], {"slab": slab, "sub": to})
            words_ref[sub] = mine[sub]
    for i in ORDER[1:]:
        origin = moved(sub, i, -1)
        expect(words_ref.at[origin], w_send.at[i], w_recv.at[i], {"slab": slab, "sub": origin})
    flat = jnp.concatenate([words_ref[j] for j in range(n_sub)], axis=0)
    brick = jnp.bitwise_and(jnp.right_shift(jnp.transpose(flat)[0:8, :], 10), 63)
    offset = jnp.bitwise_and(sub // 4 - jnp.right_shift(brick, 2), 3) * 4 + jnp.bitwise_and(sub - brick, 3)
    slot = jnp.zeros(brick.shape, jnp.int32)
    for n, i in enumerate(ORDER):
        slot = jnp.where(offset == i, n, slot)
    table_ref[...] = jnp.minimum(jnp.bitwise_and(brick, 48), 2 * n_sub) + slot
    to_smem = pltpu.make_async_copy(table_ref, table_smem, own_sem.at[0])
    to_smem.start()
    loads[3].wait()
    to_smem.wait()
    @pl.when(has_upper)
    def _():
        for first, last in GROUPS:
            expect(win_ref.at[2 * n_sub + first : 2 * n_sub + last], lo_send.at[first], lo_recv.at[first], {"slab": upper, "sub": sub})

    @pl.when(has_lower)
    def _():
        for first, last in GROUPS:
            expect(win_ref.at[first:last], hi_send.at[first], hi_recv.at[first], {"slab": lower, "sub": sub})

    def columns_of(b, k):
        word = words_ref[b][k : k + 1, :]
        local = jnp.broadcast_to(jnp.bitwise_and(word, 127), (rows, cells))
        which = jnp.broadcast_to(jnp.bitwise_and(jnp.right_shift(word, 8), 3), (rows, cells)).astype(jnp.int16)
        there = jnp.broadcast_to(jnp.bitwise_and(word, 128), (rows, cells)).astype(jnp.int16)
        merged = win_ref[table_smem[0, b * 16 + k]]
        for c in range(1, 4):
            merged = jnp.where(which == c, win_ref[table_smem[c, b * 16 + k]], merged)
        got = jnp.take_along_axis(merged.astype(F32), local, axis=1, mode="promise_in_bounds").astype(BF16)
        return jnp.where(there != 0, got, jnp.zeros((), BF16))

    def part_copy(i, target):
        return pltpu.make_async_remote_copy(
            src_ref=part_ref.at[i], dst_ref=got.at[i], send_sem=p_send.at[i], recv_sem=p_recv.at[i],
            device_id={"slab": slab, "sub": target}, device_id_type=MESH,
        )

    def two_bricks(n, carry):
        ids = [15 - 2 * n, 14 - 2 * n]
        bricks = [moved(sub, i, 1) for i in ids]
        total = jnp.zeros((rows, 2 * cells), F32)
        for k in range(per):
            both = jnp.concatenate([columns_of(b, k) for b in bricks], axis=1)
            total += jnp.dot(ops_ref[k], both, preferred_element_type=F32)
        for q, (i, b) in enumerate(zip(ids, bricks)):
            part_ref[i] = total[:, q * cells : (q + 1) * cells].astype(BF16)

            @pl.when(i != 0)
            def _():
                part_copy(i, b).start()

        return carry

    lax.fori_loop(0, n_sub // 2, two_bricks, 0)
    loads[4].wait()
    total = part_ref[0].astype(F32)
    for i in reversed(ORDER[1:]):
        part_copy(i, moved(sub, i, -1)).wait_recv()
        total += got[i].astype(F32)
    locals_all = (incoming_ref[...].astype(F32) + total).astype(BF16)
    loads[5].wait()
    wide = 2 * cells
    stores = []
    for g in range(8 * cells // wide):
        row = lax.broadcasted_iota(jnp.int32, (cells, wide), 0)
        column = lax.broadcasted_iota(jnp.int32, (cells, wide), 1) + g * wide
        spread = jnp.where(jnp.right_shift(column, 3) == row, 1.0, 0.0).astype(BF16)
        repeated = jnp.dot(locals_all, spread, preferred_element_type=F32)
        octant = jnp.bitwise_and(lax.broadcasted_iota(jnp.int32, repeated.shape, 1), 7)
        result = jnp.zeros(repeated.shape, F32)
        for o in range(8):
            kept = jnp.where(octant == o, repeated, 0.0).astype(BF16)
            result += jnp.dot(l2l_ref[o], kept, preferred_element_type=F32)
        result_ref[:, g * wide : (g + 1) * wide] = result
        columns = pl.ds(g * wide, wide)
        stores.append(pltpu.make_async_copy(result_ref.at[:, columns], out_hbm.at[:, columns], out_sem.at[g]))
        stores[-1].start()
    for store in stores:
        store.wait()
    for i in ORDER[1:]:
        part_copy(i, moved(sub, i, 1)).wait_send()
    for first, last in GROUPS:
        for has, copy in beside_copies(first, last):
            pl.when(has)(copy.wait_send)
    for copy in copies:
        copy.wait_send()


def solution(mesh):
    n_slab, n_sub = mesh.shape["slab"], mesh.shape["sub"]
    dma = pltpu.SemaphoreType.DMA

    def local(child_moments, incoming, m2m_ops, m2l_ops, l2l_ops, partners):
        rows = child_moments.shape[0]
        cells = incoming.shape[1]
        per = m2l_ops.shape[0]
        args = (child_moments, incoming, m2m_ops, m2l_ops, l2l_ops, partners)
        return pl.pallas_call(
            functools.partial(main_kernel, n_slab, n_sub, per),
            name="main",
            out_shape=jax.ShapeDtypeStruct((rows, 8 * cells), F32),
            in_specs=[HB] * 6,
            out_specs=HB,
            scratch_shapes=[pltpu.VMEM(a.shape, a.dtype) for a in args]
            + [
                dma((6,)),
                pltpu.VMEM((rows, cells), BF16),
                pltpu.VMEM((3 * n_sub, rows, cells), BF16),
                pltpu.VMEM((n_sub, 16, cells), jnp.int32),
                pltpu.VMEM((n_sub, 16, cells), jnp.int32),
                pltpu.VMEM((8, n_sub * 16), jnp.int32),
                pltpu.SMEM((8, n_sub * 16), jnp.int32),
                pltpu.VMEM((n_sub, rows, cells), BF16),
                pltpu.VMEM((n_sub, rows, cells), BF16),
            ]
            + [dma((16,))] * 4
            + [dma((2, 16))] * 2
            + [dma((16,))] * 6
            + [dma((1,)), pltpu.VMEM((rows, 8 * cells), F32), dma((4,))],
            compiler_params=pltpu.CompilerParams(collective_id=0, has_side_effects=True, vmem_limit_bytes=LIMIT),
        )(*args)

    in_specs = (
        P(None, ("slab", "sub")),
        P(None, ("slab", "sub")),
        P(),
        P("sub", None, None),
        P(),
        P(None, ("slab", "sub")),
    )
    return jax.shard_map(local, mesh=mesh, in_specs=in_specs, out_specs=P(None, ("slab", "sub")), check_vma=False)
```

```python
import functools

import jax
import jax.numpy as jnp
from jax import lax
from jax.experimental import pallas as pl
from jax.experimental.pallas import tpu as pltpu
from jax.sharding import PartitionSpec as P

MESH = pl.DeviceIdType.MESH
F32 = jnp.float32
BF16 = jnp.bfloat16
VM = pl.BlockSpec(memory_space=pltpu.VMEM)
HB = pl.BlockSpec(memory_space=pltpu.HBM)
NONE = 64
LIMIT = 66_200_000


ORDER = [0, 4, 12, 1, 3, 8, 2, 5, 7, 13, 15, 9, 11, 6, 14, 10]
GROUPS = [(0, 1), (1, 3), (3, 5), (5, 7), (7, 9), (9, 11), (11, 13), (13, 15), (15, 16)]
AXES = ORDER[1:7]
SPLIT = 112


def moved(sub, i, sign):
    x, y = sub // 4, sub % 4
    return (x + sign * (i // 4) + 4) % 4 * 4 + (y + sign * (i % 4) + 4) % 4


def main_kernel(n_slab, n_sub, per, child_hbm, incoming_hbm, m2m_hbm, ops_hbm, l2l_hbm, partners_hbm, out_hbm,
                child_ref, incoming_ref, m2m_ref, ops_ref, l2l_ref, partners_ref, in_sem,
                block, win_ref, mine, words_ref, table_ref, table_smem, part_ref, got,
                w_send, w_recv, b_send, b_recv, h_send, h_recv, lo_send, lo_recv, hi_send, hi_recv, p_send, p_recv, own_sem, result_ref, out_sem):
    slab = lax.axis_index("slab")
    sub = lax.axis_index("sub")
    lower = (slab + n_slab - 1) % n_slab
    upper = (slab + 1) % n_slab
    rows, cells = block.shape

    loads = [
        pltpu.make_async_copy(source, target, in_sem.at[i])
        for i, (source, target) in enumerate(
            [(child_hbm, child_ref), (m2m_hbm, m2m_ref), (partners_hbm, partners_ref), (ops_hbm, ops_ref), (incoming_hbm, incoming_ref), (l2l_hbm, l2l_ref)]
        )
    ]
    for load in loads:
        load.start()
    barrier = pltpu.get_barrier_semaphore()
    for i in range(1, n_sub):
        pl.semaphore_signal(barrier, inc=1, device_id={"slab": slab, "sub": moved(sub, i, 1)}, device_id_type=MESH)
    has_lower, has_upper = slab > 0, slab < n_slab - 1
    for has, other in ((has_lower, lower), (has_upper, upper)):

        @pl.when(has)
        def _():
            pl.semaphore_signal(barrier, inc=1, device_id={"slab": other, "sub": sub}, device_id_type=MESH)

    for has, edge in ((has_lower, 0), (has_upper, 2 * n_sub)):

        @pl.when(jnp.logical_not(has))
        def _():
            win_ref[edge : edge + n_sub] = jnp.zeros((n_sub, rows, cells), BF16)

    source = lax.broadcasted_iota(jnp.int32, (256, 256), 0)
    lane = lax.broadcasted_iota(jnp.int32, (256, 256), 1)
    picks = []
    for h in range(4):
        o = jnp.bitwise_and(jnp.right_shift(lane, 5) - h, 3) + jnp.bitwise_and(jnp.right_shift(lane, 5), 4)
        picks.append(jnp.where(source == 8 * jnp.bitwise_and(lane, 31) + o, 1.0, 0.0).astype(BF16))
    loads[0].wait()
    spread = [jnp.dot(child_ref[:, 256 * h : 256 * (h + 1)], picks[h], preferred_element_type=F32).astype(BF16) for h in range(4)]
    loads[1].wait()
    quarter = lax.broadcasted_iota(jnp.int32, (rows, cells), 1) // 32
    total = jnp.zeros((rows, cells), F32)
    for r in range(4):
        turned = jnp.zeros((rows, cells), F32)
        for o in (r, r + 4):
            half = [piece[:, cells * (o // 4) : cells * (o // 4 + 1)].astype(F32) for piece in spread]
            column = half[(0 - r) % 4]
            for q in range(1, 4):
                column = jnp.where(quarter == q, half[(q - r) % 4], column)
            turned += jnp.dot(m2m_ref[o], column.astype(BF16), preferred_element_type=F32)
        total += turned if r == 0 else pltpu.roll(turned, cells - 32 * r, 1)
    moments = total.astype(BF16)
    block[...] = moments
    win_ref[n_sub] = moments
    pl.semaphore_wait(barrier, n_sub - 1 + jnp.minimum(slab, 1) + jnp.minimum(n_slab - 1 - slab, 1))

    copies = []

    def send(src, dst, send_sem, recv_sem, device):
        copy = pltpu.make_async_remote_copy(
            src_ref=src, dst_ref=dst, send_sem=send_sem, recv_sem=recv_sem, device_id=device, device_id_type=MESH
        )
        copy.start()
        copies.append(copy)

    def expect(dst, send_sem, recv_sem, device):
        pltpu.make_async_remote_copy(
            src_ref=dst, dst_ref=dst, send_sem=send_sem, recv_sem=recv_sem, device_id=device, device_id_type=MESH
        ).wait_recv()

    def beside_copies(first, last):
        return [
            (
                has,
                pltpu.make_async_remote_copy(
                    src_ref=win_ref.at[n_sub + first : n_sub + last], dst_ref=win_ref.at[place + first : place + last],
                    send_sem=sends.at[first], recv_sem=recvs.at[first], device_id={"slab": device, "sub": sub}, device_id_type=MESH,
                ),
            )
            for has, device, place, sends, recvs in (
                (has_lower, lower, 2 * n_sub, lo_send, lo_recv), (has_upper, upper, 0, hi_send, hi_recv)
            )
        ]

    def beside(first, last):
        for has, copy in beside_copies(first, last):
            pl.when(has)(copy.start)

    beside(0, 1)
    for i in AXES:
        send(block, win_ref.at[n_sub + ORDER.index(i)], b_send.at[i], b_recv.at[i], {"slab": slab, "sub": moved(sub, i, 1)})
    halves = (pl.ds(0, SPLIT), pl.ds(SPLIT, rows - SPLIT))

    loads[2].wait()
    base = (slab - 1) * (n_sub * cells)
    lane = lax.broadcasted_iota(jnp.int32, (per, cells), 1)
    place = lax.broadcasted_iota(jnp.int32, (cells, cells), 0)
    across = lax.broadcasted_iota(jnp.int32, (cells, cells), 1)

    def words_for(group):
        codes, tables, which_of = [], [], []
        for j in range(8 * group, 8 * group + 8):
            p = partners_ref[per * j : per * (j + 1), :]
            rel = p - base
            brick = jnp.where(p >= 0, jnp.right_shift(rel, 7), NONE)
            which = jnp.zeros(p.shape, jnp.int32)
            packed = jnp.zeros(p.shape, jnp.int32)
            last = jnp.full((per, 1), -1, jnp.int32)
            for c in range(4):
                last = jnp.min(jnp.where(brick > last, brick, NONE), axis=1, keepdims=True)
                which = jnp.where((brick == last) & (brick < NONE), c, which)
                packed = jnp.where(lane % 4 == c, jnp.where(last < NONE, last, n_sub), packed)
            codes.append(jnp.where(p >= 0, jnp.bitwise_and(rel, 127) + 128, 0))
            tables.append(packed)
            which_of.append(which.astype(F32))
            which_of.append(jnp.zeros((16 - per, cells), F32))
        turned = jnp.transpose(jnp.concatenate(which_of, axis=0))
        back = jnp.zeros((cells, cells), F32)
        for j in range(8):
            left, right = [], []
            for k in range(per):
                left.append(jnp.where(jnp.bitwise_and(codes[j][k : k + 1, :], 127) == place, 1.0, 0.0).astype(BF16))
                right.append(jnp.where(across == 16 * j + k, turned, 0.0).astype(BF16))
            back += jnp.dot(jnp.concatenate(left, axis=1), jnp.concatenate(right, axis=0), preferred_element_type=F32)
        back = jnp.transpose(back).astype(jnp.int32)
        for j in range(8):
            mine[8 * group + j, 0:per, :] = codes[j] + jnp.bitwise_and(back[16 * j : 16 * j + per, :], 3) * 256 + tables[j] * 1024
            mine[8 * group + j, per:16, :] = jnp.zeros((16 - per, cells), jnp.int32)

    words_for(0)
    for first, last in GROUPS[1:]:
        for n in range(first, last):
            i = ORDER[n]
            origin = {"slab": slab, "sub": moved(sub, i, -1)}
            landed = win_ref.at[n_sub + n]
            if i in AXES:
                expect(landed, b_send.at[i], b_recv.at[i], origin)
                half, onward = (0, (1, 3, 2)) if i % 4 == 0 else (1, (4, 12, 8))
                for step in onward:
                    m = ORDER.index(i + step)
                    send(
                        landed.at[halves[half]], win_ref.at[n_sub + m, halves[half]], h_send.at[half, i + step], h_recv.at[half, i + step],
                        {"slab": slab, "sub": moved(sub, step, 1)},
                    )
            else:
                for half in range(2):
                    expect(landed.at[halves[half]], h_send.at[half, i], h_recv.at[half, i], origin)
        beside(first, last)
        if last == 7:
            words_for(1)
            for i in reversed(ORDER[1:]):
                to = moved(sub, i, 1)
                send(mine.at[to], words_ref.at[sub], w_send.at[i], w_recv.at[i], {"slab": slab, "sub": to})
            words_ref[sub] = mine[sub]
    for i in ORDER[1:]:
        origin = moved(sub, i, -1)
        expect(words_ref.at[origin], w_send.at[i], w_recv.at[i], {"slab": slab, "sub": origin})
    flat = jnp.concatenate([words_ref[j] for j in range(n_sub)], axis=0)
    brick = jnp.bitwise_and(jnp.right_shift(jnp.transpose(flat)[0:8, :], 10), 63)
    offset = jnp.bitwise_and(sub // 4 - jnp.right_shift(brick, 2), 3) * 4 + jnp.bitwise_and(sub - brick, 3)
    slot = jnp.zeros(brick.shape, jnp.int32)
    for n, i in enumerate(ORDER):
        slot = jnp.where(offset == i, n, slot)
    table_ref[...] = jnp.minimum(jnp.bitwise_and(brick, 48), 2 * n_sub) + slot
    to_smem = pltpu.make_async_copy(table_ref, table_smem, own_sem.at[0])
    to_smem.start()
    loads[3].wait()
    to_smem.wait()
    @pl.when(has_upper)
    def _():
        for first, last in GROUPS:
            expect(win_ref.at[2 * n_sub + first : 2 * n_sub + last], lo_send.at[first], lo_recv.at[first], {"slab": upper, "sub": sub})

    @pl.when(has_lower)
    def _():
        for first, last in GROUPS:
            expect(win_ref.at[first:last], hi_send.at[first], hi_recv.at[first], {"slab": lower, "sub": sub})

    def columns_of(b, k):
        word = words_ref[b][k : k + 1, :]
        local = jnp.broadcast_to(jnp.bitwise_and(word, 127), (rows, cells))
        which = jnp.broadcast_to(jnp.bitwise_and(jnp.right_shift(word, 8), 3), (rows, cells)).astype(jnp.int16)
        there = jnp.broadcast_to(jnp.bitwise_and(word, 128), (rows, cells)).astype(jnp.int16)
        merged = win_ref[table_smem[0, b * 16 + k]]
        for c in range(1, 4):
            merged = jnp.where(which == c, win_ref[table_smem[c, b * 16 + k]], merged)
        got = jnp.take_along_axis(merged.astype(F32), local, axis=1, mode="promise_in_bounds").astype(BF16)
        return jnp.where(there != 0, got, jnp.zeros((), BF16))

    def part_copy(i, target):
        return pltpu.make_async_remote_copy(
            src_ref=part_ref.at[i], dst_ref=got.at[i], send_sem=p_send.at[i], recv_sem=p_recv.at[i],
            device_id={"slab": slab, "sub": target}, device_id_type=MESH,
        )

    def two_bricks(n, carry):
        ids = [jnp.bitwise_and(jnp.right_shift(jnp.int32(digits), 4 * n), 15) for digits in (0x4185D96A, 0x0C327FBE)]
        bricks = [moved(sub, i, 1) for i in ids]
        total = jnp.zeros((rows, 2 * cells), F32)
        for k in range(per):
            both = jnp.concatenate([columns_of(b, k) for b in bricks], axis=1)
            total += jnp.dot(ops_ref[k], both, preferred_element_type=F32)
        for q, (i, b) in enumerate(zip(ids, bricks)):
            part_ref[i] = total[:, q * cells : (q + 1) * cells].astype(BF16)

            @pl.when(i != 0)
            def _():
                part_copy(i, b).start()

        return carry

    lax.fori_loop(0, n_sub // 2, two_bricks, 0)
    loads[4].wait()
    total = part_ref[0].astype(F32)
    for i in reversed(ORDER[1:]):
        part_copy(i, moved(sub, i, -1)).wait_recv()
        total += got[i].astype(F32)
    locals_all = (incoming_ref[...].astype(F32) + total).astype(BF16)
    loads[5].wait()
    rolled = [pltpu.roll(locals_all.astype(F32), 32 * r, 1).astype(BF16) if r else locals_all for r in range(4)]
    octants = [jnp.dot(l2l_ref[o], rolled[o % 4], preferred_element_type=F32) for o in range(8)]
    wide = 2 * cells
    stores = []
    lane = lax.broadcasted_iota(jnp.int32, (wide, wide), 0)
    column = lax.broadcasted_iota(jnp.int32, (wide, wide), 1)
    for g in range(8 * cells // wide):
        o = jnp.bitwise_and(jnp.right_shift(lane, 5) - g, 3) + jnp.bitwise_and(jnp.right_shift(lane, 5), 4)
        spread = jnp.where(column == 8 * jnp.bitwise_and(lane, 31) + o, 1.0, 0.0).astype(BF16)
        both = []
        for half in range(2):
            mixed = octants[(0 - g) % 4 + 4 * half]
            for q in range(1, 4):
                mixed = jnp.where(quarter == q, octants[(q - g) % 4 + 4 * half], mixed)
            both.append(mixed)
        mixed = jnp.concatenate(both, axis=1)
        high = mixed.astype(BF16)
        low = (mixed - high.astype(F32)).astype(BF16)
        result = jnp.dot(high, spread, preferred_element_type=F32) + jnp.dot(low, spread, preferred_element_type=F32)
        result_ref[:, g * wide : (g + 1) * wide] = result
        columns = pl.ds(g * wide, wide)
        stores.append(pltpu.make_async_copy(result_ref.at[:, columns], out_hbm.at[:, columns], out_sem.at[g]))
        stores[-1].start()
    for store in stores:
        store.wait()
    for i in ORDER[1:]:
        part_copy(i, moved(sub, i, 1)).wait_send()
    for first, last in GROUPS:
        for has, copy in beside_copies(first, last):
            pl.when(has)(copy.wait_send)
    for copy in copies:
        copy.wait_send()


def solution(mesh):
    n_slab, n_sub = mesh.shape["slab"], mesh.shape["sub"]
    dma = pltpu.SemaphoreType.DMA

    def local(child_moments, incoming, m2m_ops, m2l_ops, l2l_ops, partners):
        rows = child_moments.shape[0]
        cells = incoming.shape[1]
        per = m2l_ops.shape[0]
        args = (child_moments, incoming, m2m_ops, m2l_ops, l2l_ops, partners)
        return pl.pallas_call(
            functools.partial(main_kernel, n_slab, n_sub, per),
            name="main",
            out_shape=jax.ShapeDtypeStruct((rows, 8 * cells), F32),
            in_specs=[HB] * 6,
            out_specs=HB,
            scratch_shapes=[pltpu.VMEM(a.shape, a.dtype) for a in args]
            + [
                dma((6,)),
                pltpu.VMEM((rows, cells), BF16),
                pltpu.VMEM((3 * n_sub, rows, cells), BF16),
                pltpu.VMEM((n_sub, 16, cells), jnp.int32),
                pltpu.VMEM((n_sub, 16, cells), jnp.int32),
                pltpu.VMEM((8, n_sub * 16), jnp.int32),
                pltpu.SMEM((8, n_sub * 16), jnp.int32),
                pltpu.VMEM((n_sub, rows, cells), BF16),
                pltpu.VMEM((n_sub, rows, cells), BF16),
            ]
            + [dma((16,))] * 4
            + [dma((2, 16))] * 2
            + [dma((16,))] * 6
            + [dma((1,)), pltpu.VMEM((rows, 8 * cells), F32), dma((4,))],
            compiler_params=pltpu.CompilerParams(collective_id=0, has_side_effects=True, vmem_limit_bytes=LIMIT),
        )(*args)

    in_specs = (
        P(None, ("slab", "sub")),
        P(None, ("slab", "sub")),
        P(),
        P("sub", None, None),
        P(),
        P(None, ("slab", "sub")),
    )
    return jax.shard_map(local, mesh=mesh, in_specs=in_specs, out_specs=P(None, ("slab", "sub")), check_vma=False)
```

```python
import functools

import jax
import jax.numpy as jnp
from jax import lax
from jax.experimental import pallas as pl
from jax.experimental.pallas import tpu as pltpu
from jax.sharding import PartitionSpec as P

MESH = pl.DeviceIdType.MESH
F32 = jnp.float32
BF16 = jnp.bfloat16
VM = pl.BlockSpec(memory_space=pltpu.VMEM)
HB = pl.BlockSpec(memory_space=pltpu.HBM)
NONE = 64
LIMIT = 66_200_000


ORDER = [0, 4, 12, 1, 3, 8, 2, 5, 7, 13, 15, 9, 11, 6, 14, 10]
GROUPS = [(0, 1), (1, 5), (5, 7), (7, 11), (11, 15), (15, 16)]
AXES = ORDER[1:7]
SPLIT = 112


def moved(sub, i, sign):
    x, y = sub // 4, sub % 4
    return (x + sign * (i // 4) + 4) % 4 * 4 + (y + sign * (i % 4) + 4) % 4


def main_kernel(n_slab, n_sub, per, child_hbm, incoming_hbm, m2m_hbm, ops_hbm, l2l_hbm, partners_hbm, out_hbm,
                child_ref, incoming_ref, m2m_ref, ops_ref, l2l_ref, partners_ref, in_sem,
                block, win_ref, mine, words_ref, table_ref, table_smem, part_ref, got,
                w_send, w_recv, b_send, b_recv, h_send, h_recv, lo_send, lo_recv, hi_send, hi_recv, p_send, p_recv, own_sem, result_ref, out_sem):
    slab = lax.axis_index("slab")
    sub = lax.axis_index("sub")
    lower = (slab + n_slab - 1) % n_slab
    upper = (slab + 1) % n_slab
    rows, cells = block.shape

    loads = [
        pltpu.make_async_copy(source, target, in_sem.at[i])
        for i, (source, target) in enumerate(
            [(child_hbm, child_ref), (m2m_hbm, m2m_ref), (partners_hbm, partners_ref), (ops_hbm, ops_ref), (incoming_hbm, incoming_ref), (l2l_hbm, l2l_ref)]
        )
    ]
    for load in loads:
        load.start()
    barrier = pltpu.get_barrier_semaphore()
    for i in range(1, n_sub):
        pl.semaphore_signal(barrier, inc=1, device_id={"slab": slab, "sub": moved(sub, i, 1)}, device_id_type=MESH)
    has_lower, has_upper = slab > 0, slab < n_slab - 1
    for has, other in ((has_lower, lower), (has_upper, upper)):

        @pl.when(has)
        def _():
            pl.semaphore_signal(barrier, inc=1, device_id={"slab": other, "sub": sub}, device_id_type=MESH)

    for has, edge in ((has_lower, 0), (has_upper, 2 * n_sub)):

        @pl.when(jnp.logical_not(has))
        def _():
            win_ref[edge : edge + n_sub] = jnp.zeros((n_sub, rows, cells), BF16)

    source = lax.broadcasted_iota(jnp.int32, (256, 256), 0)
    lane = lax.broadcasted_iota(jnp.int32, (256, 256), 1)
    picks = []
    for h in range(4):
        o = jnp.bitwise_and(jnp.right_shift(lane, 5) - h, 3) + jnp.bitwise_and(jnp.right_shift(lane, 5), 4)
        picks.append(jnp.where(source == 8 * jnp.bitwise_and(lane, 31) + o, 1.0, 0.0).astype(BF16))
    loads[0].wait()
    spread = [jnp.dot(child_ref[:, 256 * h : 256 * (h + 1)], picks[h], preferred_element_type=F32).astype(BF16) for h in range(4)]
    loads[1].wait()
    quarter = lax.broadcasted_iota(jnp.int32, (rows, cells), 1) // 32
    total = jnp.zeros((rows, cells), F32)
    for r in range(4):
        turned = jnp.zeros((rows, cells), F32)
        for o in (r, r + 4):
            half = [piece[:, cells * (o // 4) : cells * (o // 4 + 1)].astype(F32) for piece in spread]
            column = half[(0 - r) % 4]
            for q in range(1, 4):
                column = jnp.where(quarter == q, half[(q - r) % 4], column)
            turned += jnp.dot(m2m_ref[o], column.astype(BF16), preferred_element_type=F32)
        total += turned if r == 0 else pltpu.roll(turned, cells - 32 * r, 1)
    moments = total.astype(BF16)
    block[...] = moments
    win_ref[n_sub] = moments
    pl.semaphore_wait(barrier, n_sub - 1 + jnp.minimum(slab, 1) + jnp.minimum(n_slab - 1 - slab, 1))

    copies = []

    def send(src, dst, send_sem, recv_sem, device):
        copy = pltpu.make_async_remote_copy(
            src_ref=src, dst_ref=dst, send_sem=send_sem, recv_sem=recv_sem, device_id=device, device_id_type=MESH
        )
        copy.start()
        copies.append(copy)

    def expect(dst, send_sem, recv_sem, device):
        pltpu.make_async_remote_copy(
            src_ref=dst, dst_ref=dst, send_sem=send_sem, recv_sem=recv_sem, device_id=device, device_id_type=MESH
        ).wait_recv()

    def beside_copies(first, last):
        return [
            (
                has,
                pltpu.make_async_remote_copy(
                    src_ref=win_ref.at[n_sub + first : n_sub + last], dst_ref=win_ref.at[place + first : place + last],
                    send_sem=sends.at[first], recv_sem=recvs.at[first], device_id={"slab": device, "sub": sub}, device_id_type=MESH,
                ),
            )
            for has, device, place, sends, recvs in (
                (has_lower, lower, 2 * n_sub, lo_send, lo_recv), (has_upper, upper, 0, hi_send, hi_recv)
            )
        ]

    def beside(first, last):
        for has, copy in beside_copies(first, last):
            pl.when(has)(copy.start)

    beside(0, 1)
    for i in AXES:
        send(block, win_ref.at[n_sub + ORDER.index(i)], b_send.at[i], b_recv.at[i], {"slab": slab, "sub": moved(sub, i, 1)})
    halves = (pl.ds(0, SPLIT), pl.ds(SPLIT, rows - SPLIT))

    loads[2].wait()
    base = (slab - 1) * (n_sub * cells)
    lane = lax.broadcasted_iota(jnp.int32, (per, cells), 1)
    place = lax.broadcasted_iota(jnp.int32, (cells, cells), 0)
    across = lax.broadcasted_iota(jnp.int32, (cells, cells), 1)

    def words_for(group):
        codes, tables, which_of = [], [], []
        for j in range(8 * group, 8 * group + 8):
            p = partners_ref[per * j : per * (j + 1), :]
            rel = p - base
            brick = jnp.where(p >= 0, jnp.right_shift(rel, 7), NONE)
            which = jnp.zeros(p.shape, jnp.int32)
            packed = jnp.zeros(p.shape, jnp.int32)
            last = jnp.full((per, 1), -1, jnp.int32)
            for c in range(4):
                last = jnp.min(jnp.where(brick > last, brick, NONE), axis=1, keepdims=True)
                which = jnp.where((brick == last) & (brick < NONE), c, which)
                packed = jnp.where(lane % 4 == c, jnp.where(last < NONE, last, n_sub), packed)
            codes.append(jnp.where(p >= 0, jnp.bitwise_and(rel, 127) + 128, 0))
            tables.append(packed)
            which_of.append(which.astype(F32))
            which_of.append(jnp.zeros((16 - per, cells), F32))
        turned = jnp.transpose(jnp.concatenate(which_of, axis=0))
        back = jnp.zeros((cells, cells), F32)
        for j in range(8):
            left, right = [], []
            for k in range(per):
                left.append(jnp.where(jnp.bitwise_and(codes[j][k : k + 1, :], 127) == place, 1.0, 0.0).astype(BF16))
                right.append(jnp.where(across == 16 * j + k, turned, 0.0).astype(BF16))
            back += jnp.dot(jnp.concatenate(left, axis=1), jnp.concatenate(right, axis=0), preferred_element_type=F32)
        back = jnp.transpose(back).astype(jnp.int32)
        for j in range(8):
            mine[8 * group + j, 0:per, :] = codes[j] + jnp.bitwise_and(back[16 * j : 16 * j + per, :], 3) * 256 + tables[j] * 1024
            mine[8 * group + j, per:16, :] = jnp.zeros((16 - per, cells), jnp.int32)

    words_for(0)
    for first, last in GROUPS[1:]:
        for n in range(first, last):
            i = ORDER[n]
            origin = {"slab": slab, "sub": moved(sub, i, -1)}
            landed = win_ref.at[n_sub + n]
            if i in AXES:
                expect(landed, b_send.at[i], b_recv.at[i], origin)
                half, onward = (0, (1, 3, 2)) if i % 4 == 0 else (1, (4, 12, 8))
                for step in onward:
                    m = ORDER.index(i + step)
                    send(
                        landed.at[halves[half]], win_ref.at[n_sub + m, halves[half]], h_send.at[half, i + step], h_recv.at[half, i + step],
                        {"slab": slab, "sub": moved(sub, step, 1)},
                    )
            else:
                for half in range(2):
                    expect(landed.at[halves[half]], h_send.at[half, i], h_recv.at[half, i], origin)
        beside(first, last)
        if last == 7:
            words_for(1)
            for i in reversed(ORDER[1:]):
                to = moved(sub, i, 1)
                send(mine.at[to], words_ref.at[sub], w_send.at[i], w_recv.at[i], {"slab": slab, "sub": to})
            words_ref[sub] = mine[sub]
    for i in ORDER[1:]:
        origin = moved(sub, i, -1)
        expect(words_ref.at[origin], w_send.at[i], w_recv.at[i], {"slab": slab, "sub": origin})
    flat = jnp.concatenate([words_ref[j] for j in range(n_sub)], axis=0)
    brick = jnp.bitwise_and(jnp.right_shift(jnp.transpose(flat)[0:8, :], 10), 63)
    offset = jnp.bitwise_and(sub // 4 - jnp.right_shift(brick, 2), 3) * 4 + jnp.bitwise_and(sub - brick, 3)
    slot = jnp.zeros(brick.shape, jnp.int32)
    for n, i in enumerate(ORDER):
        slot = jnp.where(offset == i, n, slot)
    table_ref[...] = jnp.minimum(jnp.bitwise_and(brick, 48), 2 * n_sub) + slot
    to_smem = pltpu.make_async_copy(table_ref, table_smem, own_sem.at[0])
    to_smem.start()
    loads[3].wait()
    to_smem.wait()
    @pl.when(has_upper)
    def _():
        for first, last in GROUPS:
            expect(win_ref.at[2 * n_sub + first : 2 * n_sub + last], lo_send.at[first], lo_recv.at[first], {"slab": upper, "sub": sub})

    @pl.when(has_lower)
    def _():
        for first, last in GROUPS:
            expect(win_ref.at[first:last], hi_send.at[first], hi_recv.at[first], {"slab": lower, "sub": sub})

    def columns_of(b, k):
        word = words_ref[b][k : k + 1, :]
        local = jnp.broadcast_to(jnp.bitwise_and(word, 127), (rows, cells))
        which = jnp.broadcast_to(jnp.bitwise_and(jnp.right_shift(word, 8), 3), (rows, cells)).astype(jnp.int16)
        there = jnp.broadcast_to(jnp.bitwise_and(word, 128), (rows, cells)).astype(jnp.int16)
        merged = win_ref[table_smem[0, b * 16 + k]]
        for c in range(1, 4):
            merged = jnp.where(which == c, win_ref[table_smem[c, b * 16 + k]], merged)
        got = jnp.take_along_axis(merged.astype(F32), local, axis=1, mode="promise_in_bounds").astype(BF16)
        return jnp.where(there != 0, got, jnp.zeros((), BF16))

    def part_copy(i, target):
        return pltpu.make_async_remote_copy(
            src_ref=part_ref.at[i], dst_ref=got.at[i], send_sem=p_send.at[i], recv_sem=p_recv.at[i],
            device_id={"slab": slab, "sub": target}, device_id_type=MESH,
        )

    def two_bricks(n, carry):
        ids = [jnp.bitwise_and(jnp.right_shift(jnp.int32(digits), 4 * n), 15) for digits in (0x4185D96A, 0x0C327FBE)]
        bricks = [moved(sub, i, 1) for i in ids]
        total = jnp.zeros((rows, 2 * cells), F32)
        for k in range(per):
            both = jnp.concatenate([columns_of(b, k) for b in bricks], axis=1)
            total += jnp.dot(ops_ref[k], both, preferred_element_type=F32)
        for q, (i, b) in enumerate(zip(ids, bricks)):
            part_ref[i] = total[:, q * cells : (q + 1) * cells].astype(BF16)

            @pl.when(i != 0)
            def _():
                part_copy(i, b).start()

        return carry

    lax.fori_loop(0, n_sub // 2, two_bricks, 0)
    loads[4].wait()
    total = part_ref[0].astype(F32)
    for i in reversed(ORDER[1:]):
        part_copy(i, moved(sub, i, -1)).wait_recv()
        total += got[i].astype(F32)
    locals_all = (incoming_ref[...].astype(F32) + total).astype(BF16)
    loads[5].wait()
    rolled = [pltpu.roll(locals_all.astype(F32), 32 * r, 1).astype(BF16) if r else locals_all for r in range(4)]
    octants = [jnp.dot(l2l_ref[o], rolled[o % 4], preferred_element_type=F32) for o in range(8)]
    wide = 2 * cells
    stores = []
    lane = lax.broadcasted_iota(jnp.int32, (wide, wide), 0)
    column = lax.broadcasted_iota(jnp.int32, (wide, wide), 1)
    for g in range(8 * cells // wide):
        o = jnp.bitwise_and(jnp.right_shift(lane, 5) - g, 3) + jnp.bitwise_and(jnp.right_shift(lane, 5), 4)
        spread = jnp.where(column == 8 * jnp.bitwise_and(lane, 31) + o, 1.0, 0.0).astype(BF16)
        both = []
        for half in range(2):
            mixed = octants[(0 - g) % 4 + 4 * half]
            for q in range(1, 4):
                mixed = jnp.where(quarter == q, octants[(q - g) % 4 + 4 * half], mixed)
            both.append(mixed)
        mixed = jnp.concatenate(both, axis=1)
        high = mixed.astype(BF16)
        low = (mixed - high.astype(F32)).astype(BF16)
        result = jnp.dot(high, spread, preferred_element_type=F32) + jnp.dot(low, spread, preferred_element_type=F32)
        result_ref[:, g * wide : (g + 1) * wide] = result
        columns = pl.ds(g * wide, wide)
        stores.append(pltpu.make_async_copy(result_ref.at[:, columns], out_hbm.at[:, columns], out_sem.at[g]))
        stores[-1].start()
    for store in stores:
        store.wait()
    for i in ORDER[1:]:
        part_copy(i, moved(sub, i, 1)).wait_send()
    for first, last in GROUPS:
        for has, copy in beside_copies(first, last):
            pl.when(has)(copy.wait_send)
    for copy in copies:
        copy.wait_send()


def solution(mesh):
    n_slab, n_sub = mesh.shape["slab"], mesh.shape["sub"]
    dma = pltpu.SemaphoreType.DMA

    def local(child_moments, incoming, m2m_ops, m2l_ops, l2l_ops, partners):
        rows = child_moments.shape[0]
        cells = incoming.shape[1]
        per = m2l_ops.shape[0]
        args = (child_moments, incoming, m2m_ops, m2l_ops, l2l_ops, partners)
        return pl.pallas_call(
            functools.partial(main_kernel, n_slab, n_sub, per),
            name="main",
            out_shape=jax.ShapeDtypeStruct((rows, 8 * cells), F32),
            in_specs=[HB] * 6,
            out_specs=HB,
            scratch_shapes=[pltpu.VMEM(a.shape, a.dtype) for a in args]
            + [
                dma((6,)),
                pltpu.VMEM((rows, cells), BF16),
                pltpu.VMEM((3 * n_sub, rows, cells), BF16),
                pltpu.VMEM((n_sub, 16, cells), jnp.int32),
                pltpu.VMEM((n_sub, 16, cells), jnp.int32),
                pltpu.VMEM((8, n_sub * 16), jnp.int32),
                pltpu.SMEM((8, n_sub * 16), jnp.int32),
                pltpu.VMEM((n_sub, rows, cells), BF16),
                pltpu.VMEM((n_sub, rows, cells), BF16),
            ]
            + [dma((16,))] * 4
            + [dma((2, 16))] * 2
            + [dma((16,))] * 6
            + [dma((1,)), pltpu.VMEM((rows, 8 * cells), F32), dma((4,))],
            compiler_params=pltpu.CompilerParams(collective_id=0, has_side_effects=True, vmem_limit_bytes=LIMIT),
        )(*args)

    in_specs = (
        P(None, ("slab", "sub")),
        P(None, ("slab", "sub")),
        P(),
        P("sub", None, None),
        P(),
        P(None, ("slab", "sub")),
    )
    return jax.shard_map(local, mesh=mesh, in_specs=in_specs, out_specs=P(None, ("slab", "sub")), check_vma=False)
```
